256 devices in a mesh: seq: 32 (over z, y), tensor: 8 (over x, core).
Axes of the slice: x: 4, y: 4, z: 8, core: 2. Of those that a mesh axis runs over, the one named last changes fastest.
Arguments:
- layer_input: bfloat16 [8192, 4096], P('seq', 'tensor'), may hold values from -6 to 6
- norm_gain: float32 [4096], replicated, may hold values from 0.1 to 1.9
- in_weights: bfloat16 [2, 4096, 2048], P(None, None, 'tensor'), may hold values from -0.09375 to 0.09375
- conv_weight: float32 [4, 2048], P(None, 'tensor'), may hold values from -4 to 4
- conv_bias: float32 [2048], P('tensor'), may hold values from -3 to 3
- gate_weights: bfloat16 [2, 8, 256, 256], P(None, 'tensor'), may hold values from -0.375 to 0.375
- gate_bias: float32 [2, 2048], P(None, 'tensor'), may hold values from -4 to 4
- decay_rate: float32 [2048], P('tensor'), may hold values from 1e-06 to 0.03, as said below
- out_weight: bfloat16 [2048, 4096], P('tensor'), may hold values from -0.1875 to 0.1875
- mlp_gain: float32 [4096], replicated, may hold values from 0.1 to 1.9
- mlp_in: bfloat16 [2, 4096, 6144], P(None, 'seq', 'tensor'), may hold values from -0.09375 to 0.09375
- mlp_out: bfloat16 [6144, 4096], P('tensor', 'seq'), may hold values from -0.15625 to 0.15625
Outputs:
- block_output: bfloat16 [8192, 4096], P('seq', 'tensor')
The draws below stay inside these ranges and needn't reach their ends.
Inputs may be any that keep to these rules, and one draw needn't show every extreme that they name: `decay_rate`: every rate is positive.
All inputs are finite; a program needn't handle non-finite values.
Results may differ from the reference program's by a relative error of at most 0.015.
Values may be sent and summed in bfloat16 or wider, within the bound.
No kernel may reach another device: no remote copies, remote signals or barrier semaphores. Data moves between devices by JAX's collectives and lax.ppermute only.
A program may use at most 128 MiB of HBM per device.

```python
import jax
import jax.numpy as jnp
from jax import lax

D = 4096
BW = 256
BLOCKS = 8
LRU = 2048
FF = 6144
TAPS = 4
TOKENS = 8192
N_TENSOR = 8


def draw_decay_rate(key, part):
    first_key = jax.random.fold_in(jax.random.fold_in(key, 7103), 0)
    broad = jnp.exp(jax.random.uniform(first_key, (LRU,), jnp.float32, jnp.log(1e-05), jnp.log(0.03)))
    return broad.astype(jnp.float32)


def strengthened(drawn, stream_key, source, target, blocks, factor):
    def block_of(dim):
        return (jnp.arange(drawn.shape[dim]) // (drawn.shape[dim] // blocks)).reshape((-1,) + (1,) * (drawn.ndim - 1 - dim))

    first = jax.random.permutation(stream_key, blocks)[block_of(target)]
    other_side = (block_of(target) + blocks // 2) % blocks
    return jnp.where((block_of(source) == first) | (block_of(source) == other_side), factor * drawn, drawn)


def block_scale(stream_key, shape, pieces, smallest, top_value):
    factor_of = 1.0
    for axis_at, parts in pieces:
        heights = jax.random.uniform(jax.random.fold_in(jax.random.fold_in(stream_key, 6), axis_at), (parts,), jnp.float32, smallest / len(pieces), top_value / len(pieces))
        factor_of = factor_of * jnp.repeat(jnp.exp(heights), shape[axis_at] // parts).reshape((-1,) + (1,) * (len(shape) - 1 - axis_at))
    return factor_of


def bell_draw(stream_key, shape, spread, most, shards=(), held_as=jnp.bfloat16):
    drawn = spread * jax.random.normal(stream_key, shape, jnp.float32)
    if shards:
        drawn = drawn * block_scale(stream_key, shape, shards, -0.22, 0.18)
    return jnp.clip(drawn, -most, most).astype(held_as)


def bell_draw_with(key, shape, width, most, cuts, heavy, dtype=jnp.bfloat16):
    result = width * jax.random.normal(key, shape, jnp.float32)
    if cuts:
        result = result * block_scale(key, shape, cuts, -0.22, 0.18)
    return jnp.clip(strengthened(result, jax.random.fold_in(key, 3), *heavy), -most, most).astype(dtype)


def setup_inputs(seed: int = 0) -> dict:
    keys = jax.random.split(jax.random.key(seed), 13)
    layer_input = bell_draw(keys[0], (TOKENS, D), 1.0, 6.0, ((0, 32), (1, 8)))
    norm_gain = jnp.clip(1.0 + 0.18 * jax.random.normal(keys[1], (D,), jnp.float32), 0.1, 1.9)
    in_weights = bell_draw(keys[2], (2, D, LRU), D ** -0.5, 0.09375, ((2, 8),))
    conv_weight = bell_draw(keys[3], (TAPS, LRU), 1.0, 4.0, ((1, 8),), jnp.float32)
    conv_bias = bell_draw(keys[4], (LRU,), 0.5, 3.0, ((0, 8),), jnp.float32)
    gate_weights = bell_draw(keys[5], (2, BLOCKS, BW, BW), BW ** -0.5, 0.375, ((1, 8),))
    gate_bias = bell_draw(keys[6], (2, LRU), 1.0, 4.0, ((1, 8),), jnp.float32)
    decay_rate = draw_decay_rate(jax.random.fold_in(keys[12], 71), 0)
    out_weight = bell_draw_with(keys[8], (LRU, D), LRU ** -0.5, 0.1875, ((0, 8),), (0, 1, 8, 2.0))
    mlp_gain = jnp.clip(1.0 + 0.18 * jax.random.normal(keys[9], (D,), jnp.float32), 0.1, 1.9)
    mlp_in = bell_draw(keys[10], (2, D, FF), D ** -0.5, 0.09375, ((1, 32), (2, 8)))
    mlp_out = bell_draw_with(keys[11], (FF, D), FF ** -0.5, 0.15625, ((0, 8), (1, 32)), (0, 1, 32, 2.75))
    return dict(layer_input=layer_input, norm_gain=norm_gain, in_weights=in_weights, conv_weight=conv_weight, conv_bias=conv_bias, gate_weights=gate_weights, gate_bias=gate_bias, decay_rate=decay_rate, out_weight=out_weight, mlp_gain=mlp_gain, mlp_in=mlp_in, mlp_out=mlp_out)


def rms_scale(rows, gain):
    values = rows.astype(jnp.float32)
    mean_square = lax.optimization_barrier(jnp.mean(values * values, axis=-1, keepdims=True))
    return (values * lax.rsqrt(mean_square + 1e-06) * gain).astype(jnp.bfloat16)

def advance(state, inputs):
    decay, driven = inputs
    state = decay * state + driven
    return (state, state)

def reference(layer_input, norm_gain, in_weights, conv_weight, conv_bias, gate_weights, gate_bias, decay_rate, out_weight, mlp_gain, mlp_in, mlp_out):
    normed = rms_scale(layer_input, norm_gain)
    branch_x = jnp.dot(normed, in_weights[0], preferred_element_type=jnp.float32).astype(jnp.bfloat16)
    branch_y = jax.nn.gelu(jnp.dot(normed, in_weights[1], preferred_element_type=jnp.float32), approximate=True)
    padded = jnp.concatenate([jnp.zeros((TAPS - 1, LRU), jnp.bfloat16), branch_x], axis=0).astype(jnp.float32)
    convolved = jnp.zeros((TOKENS, LRU), jnp.float32) + conv_bias
    for tap_index in range(TAPS):
        start_row = TAPS - 1 - tap_index
        convolved = convolved + conv_weight[tap_index] * padded[start_row:start_row + TOKENS]
    conv_out = convolved.astype(jnp.bfloat16)
    blocks_in = conv_out.astype(jnp.float32).reshape(TOKENS, BLOCKS, BW)
    gate_pre = jnp.einsum('tnc,knce->ktne', blocks_in, gate_weights.astype(jnp.float32)).reshape(2, TOKENS, LRU) + gate_bias[:, None, :]
    log_decay = -8.0 * jax.nn.sigmoid(gate_pre[0]) * decay_rate
    decay = jnp.exp(log_decay)
    driven = conv_out.astype(jnp.float32) * jax.nn.sigmoid(gate_pre[1]) * jnp.sqrt(-jnp.expm1(2.0 * log_decay))
    _, states = lax.scan(advance, jnp.zeros((LRU,), jnp.float32), (decay, driven))
    mixed = (states * branch_y).astype(jnp.bfloat16)
    group = LRU // N_TENSOR
    rec_sum = jnp.zeros((TOKENS, D), jnp.float32)
    for group_index in range(N_TENSOR):
        term = jnp.dot(mixed[:, group_index * group:(group_index + 1) * group], out_weight[group_index * group:(group_index + 1) * group], preferred_element_type=jnp.float32).astype(jnp.bfloat16)
        term = lax.optimization_barrier(term)
        rec_sum = rec_sum + term.astype(jnp.float32)
    residual = (layer_input.astype(jnp.float32) + rec_sum).astype(jnp.bfloat16)
    mlp_normed = rms_scale(residual, mlp_gain)
    gate = jnp.dot(mlp_normed, mlp_in[0], preferred_element_type=jnp.float32)
    upward = jnp.dot(mlp_normed, mlp_in[1], preferred_element_type=jnp.float32)
    hidden = (jax.nn.gelu(gate, approximate=True) * upward).astype(jnp.bfloat16)
    down = jnp.dot(hidden, mlp_out, preferred_element_type=jnp.float32)
    return (residual.astype(jnp.float32) + down).astype(jnp.bfloat16)
```

```python
import functools

import jax
import jax.numpy as jnp
from jax import lax
from jax.experimental import pallas as pl
from jax.experimental.pallas import tpu as pltpu
from jax.sharding import Mesh
from jax.sharding import PartitionSpec as P

SEQ = ("z", "y")
BF16, F32 = jnp.bfloat16, jnp.float32
MIB = 1 << 20
ANY = pl.BlockSpec(memory_space=pl.ANY)
VMEM = pl.BlockSpec(memory_space=pltpu.VMEM)
SMEM = pl.BlockSpec(memory_space=pltpu.SMEM)


GROUPS = ((0,), (1, -1), (2, -2), (3, -3, 4))
OUT_ORDER = (0, 1, -1, 2, -2, 3, -3, 4)


def ring(value, axis, step):
    count = lax.axis_size(axis)
    return lax.ppermute(value, axis, [(i, (i + step) % count) for i in range(count)])


def call(body, out_shape, operands, specs, scratch, flops, limit, aliases=None):
    size = sum(a.size * a.dtype.itemsize for a in operands)
    return pl.pallas_call(
        body,
        out_shape=out_shape,
        in_specs=specs,
        out_specs=VMEM,
        scratch_shapes=scratch,
        input_output_aliases=aliases or {},
        compiler_params=pltpu.CompilerParams(vmem_limit_bytes=limit),
        cost_estimate=pl.CostEstimate(flops=flops, bytes_accessed=size, transcendentals=0),
    )(*operands)


def norm_body(by_shard, index, *refs):
    pieces, (gain, out, rows, sems) = refs[:8], refs[8:]
    copies = []
    for i, piece in enumerate(pieces):
        copies.append(pltpu.make_async_copy(piece, rows.at[index[i]], sems.at[i]))
        copies[-1].start()
    squares = jnp.zeros((rows.shape[1], 1), F32)
    for i, copy in enumerate(copies):
        copy.wait()
        block = rows[index[i]].astype(F32)
        squares = squares + jnp.sum(block * block, axis=1, keepdims=True)
    scale = lax.rsqrt(squares / out.shape[1] + 1e-06)
    for k in range(32):
        if by_shard:
            shard = index[8 + k]
            block = rows[
                shard // 4, :, pl.ds(pl.multiple_of(lax.rem(shard, 4) * 128, 128), 128)
            ]
            weight = gain[shard]
        else:
            block = rows[k // 4, :, (k % 4) * 128 : (k % 4 + 1) * 128]
            weight = gain[k]
        out[:, k * 128 : (k + 1) * 128] = (block.astype(F32) * scale * weight).astype(BF16)


def norm(pieces, index, gain, by_shard):
    tokens, width = pieces[0].shape
    return call(
        functools.partial(norm_body, by_shard),
        jax.ShapeDtypeStruct((tokens, 8 * width), BF16),
        (index, *pieces, gain.reshape(32, 1, 128)),
        [SMEM] + [ANY] * 8 + [VMEM],
        [pltpu.VMEM((8, tokens, width), BF16), pltpu.SemaphoreType.DMA((8,))],
        10_000_000,
        16 * MIB,
    )


def spread_body(index, left, right, out):
    for j in range(8):
        columns = pl.ds(pl.multiple_of(index[j] * 512, 512), 512)
        out[j] = jnp.dot(left[...], right[:, columns], preferred_element_type=F32).astype(BF16)


def spread(index, left, right):
    tokens = left.shape[0]
    return call(
        spread_body,
        jax.ShapeDtypeStruct((8, tokens, 512), BF16),
        (index, left, right),
        [SMEM, VMEM, VMEM],
        [],
        2 * tokens * right.size,
        14 * MIB,
    )


def up_body(starts, first, last, *refs):
    count = len(starts)
    left, pieces, rest = refs[0], refs[1 : 1 + count], refs[1 + count :]
    if first:
        total, sums, (buffers, sems) = None, rest[0], rest[1:]
    else:
        total, sums, (buffers, sems) = rest[0], rest[1], rest[2:]
    work = sums
    if last:
        buffers, work = buffers
    copies = []
    at = 0
    rows_of = []
    for i, piece in enumerate(pieces):
        rows = piece.shape[0]
        copies.append(
            pltpu.make_async_copy(piece, buffers.at[at : at + rows], sems.at[i])
        )
        copies[-1].start()
        rows_of.append((at, rows))
        at += rows
    width = buffers.shape[1]
    for i, (at, rows) in enumerate(rows_of):
        copies[i].wait()
        for column in range(0, width, 512):
            span = slice(column, column + 512)
            term = jnp.dot(
                left[:, starts[i] : starts[i] + rows],
                buffers[at : at + rows, span],
                preferred_element_type=F32,
            )
            if i > 0:
                work[:, span] += term
            elif first:
                work[:, span] = term
            else:
                work[:, span] = total[:, span] + term
    if last:
        half = width // 2
        for column in range(0, half, 256):
            gate = work[:, column : column + 256]
            lift = work[:, half + column : half + column + 256]
            sums[:, column : column + 256] = (
                jax.nn.gelu(gate, approximate=True) * lift
            ).astype(BF16)


def up(left, pieces, starts, total, last):
    tokens, width = left.shape[0], pieces[0].shape[1]
    rows = sum(p.shape[0] for p in pieces)
    first = total is None
    out = (
        jax.ShapeDtypeStruct((tokens, width // 2), BF16)
        if last
        else jax.ShapeDtypeStruct((tokens, width), F32)
    )
    buffers = pltpu.VMEM((rows, width), BF16)
    scratch = [buffers, pltpu.SemaphoreType.DMA((len(pieces),))]

    def body(*refs):
        if last:
            refs = (*refs[:-3], (refs[-3], refs[-2]), refs[-1])
        up_body(starts, first, last, *refs)

    if last:
        scratch = [buffers, pltpu.VMEM((tokens, width), F32), scratch[1]]
    return call(
        body,
        out,
        (left, *pieces) if first else (left, *pieces, total),
        [VMEM] + [ANY] * len(pieces) + ([] if first else [VMEM]),
        scratch,
        2 * tokens * rows * width,
        20 * MIB,
    )


def down_body(index, left, *refs):
    pieces, (out, buffers, sems) = refs[:8], refs[8:]
    copies = []
    for i, piece in enumerate(pieces):
        mine = []
        for j in range(4):
            lanes = pl.ds(pl.multiple_of(index[8 + j] * 128, 128), 128)
            copy = pltpu.make_async_copy(piece.at[j], buffers.at[i, :, lanes], sems.at[i, j])
            copy.start()
            mine.append(copy)
        copies.append(mine)
    for i in range(8):
        for copy in copies[i]:
            copy.wait()
        out[index[i]] = jnp.dot(left[...], buffers[i], preferred_element_type=F32).astype(BF16)


def down(index, left, pieces):
    tokens, inner = left.shape
    return call(
        down_body,
        jax.ShapeDtypeStruct((8, tokens, 512), BF16),
        (index, left, *pieces),
        [SMEM, VMEM] + [ANY] * 8,
        [pltpu.VMEM((8, inner, 512), BF16), pltpu.SemaphoreType.DMA((8, 4))],
        2 * tokens * inner * 4096,
        20 * MIB,
    )


def blocks_of_all(own):
    before = ring(own, "x", 1)
    after = ring(own, "x", -1)
    across = ring(before, "x", 1)
    mine = (own, before, across, after)
    return mine + tuple(ring(block, "c", 1) for block in mine)


def sum_to_owner(terms):
    other = ring(terms[4:], "c", 1)
    both = terms[:4].astype(F32) + other.astype(F32)
    half = both.shape[1] // 2
    far = both[2].astype(BF16)
    ahead = ring(far[:half], "x", 1)
    behind = ring(far[half:], "x", -1)
    to_next = jnp.concatenate([both[1, :half] + ahead.astype(F32), both[1, half:]], axis=0)
    to_last = jnp.concatenate([both[3, :half], both[3, half:] + behind.astype(F32)], axis=0)
    from_last = ring(to_next.astype(BF16), "x", 1)
    from_next = ring(to_last.astype(BF16), "x", -1)
    return both[0] + from_last.astype(F32) + from_next.astype(F32)


def chain_step(earlier, later):
    return (earlier[0] * later[0], later[0] * earlier[1] + later[1])


def shards(
    layer_input,
    norm_gain,
    in_weights,
    conv_weight,
    conv_bias,
    gate_weights,
    gate_bias,
    decay_rate,
    out_weight,
    mlp_gain,
    mlp_in,
    mlp_out,
):
    z, y, x, c = (lax.axis_index(a) for a in ("z", "y", "x", "c"))
    ints = lambda values: jnp.stack(values).astype(jnp.int32)
    block_at = [((x - k) % 4) * 2 + side for side in (c, 1 - c) for k in range(4)]
    dest_at = [((x + k) % 4) * 2 + side for side in (c, 1 - c) for k in range(4)]

    own_in = jnp.concatenate([mlp_in[0], mlp_in[1]], axis=1)
    out_up, out_down = ring(mlp_out, "y", 1), ring(mlp_out, "y", -1)
    from_z = {0: own_in}
    for k in (1, 2, 3):
        from_z[k] = ring(from_z[k - 1], "z", 1)
        from_z[-k] = ring(from_z[1 - k], "z", -1)
    from_z[4] = ring(from_z[3], "z", 1)
    out_far = ring(out_up, "y", 1)
    groups = []
    for number, offsets in enumerate(GROUPS):
        own = (
            from_z[offsets[0]]
            if len(offsets) == 1
            else jnp.concatenate([from_z[k] for k in offsets], axis=0)
        )
        before, after = ring(own, "y", 1), ring(own, "y", -1)
        if number == 3:
            far = (ring(before[:256], "y", 1), ring(after[256:], "y", -1))
        elif number % 2:
            far = (ring(before, "y", 1),)
        else:
            far = (ring(after, "y", -1),)
        groups.append((own, before, after, *far))
    out_own = jnp.stack([mlp_out, out_up, out_far, out_down])
    out_z = {0: out_own}
    for k in (1, 2, 3):
        out_z[k] = ring(out_z[k - 1], "z", 1)
        out_z[-k] = ring(out_z[1 - k], "z", -1)
    out_z[4] = ring(out_z[-3], "z", -1)

    normed = norm(blocks_of_all(layer_input), ints(block_at), norm_gain, False)
    branch_x = jnp.dot(normed, in_weights[0], preferred_element_type=F32).astype(BF16)
    branch_y = jax.nn.gelu(
        jnp.dot(normed, in_weights[1], preferred_element_type=F32), approximate=True
    )
    num_tokens = branch_x.shape[0]
    rim_rows = conv_weight.shape[0] - 1
    earlier_rows = lax.ppermute(
        branch_x[num_tokens - rim_rows :], SEQ, [(i, i + 1) for i in range(31)]
    )
    padded = jnp.concatenate([earlier_rows, branch_x], axis=0).astype(F32)
    convolved = jnp.zeros(branch_x.shape, F32) + conv_bias
    for tap_index in range(conv_weight.shape[0]):
        start_row = rim_rows - tap_index
        convolved = convolved + conv_weight[tap_index] * padded[start_row : start_row + num_tokens]
    conv_out = convolved.astype(BF16)
    gate_pre = [
        jnp.dot(conv_out, gate_weights[g, 0], preferred_element_type=F32) + gate_bias[g]
        for g in range(2)
    ]
    log_decay = -8.0 * jax.nn.sigmoid(gate_pre[0]) * decay_rate
    decay = jnp.exp(log_decay)
    driven = (
        conv_out.astype(F32)
        * jax.nn.sigmoid(gate_pre[1])
        * jnp.sqrt(-jnp.expm1(2.0 * log_decay))
    )
    cum_decay, cum_state = lax.associative_scan(chain_step, (decay, driven), axis=0)
    ends = jnp.concatenate([cum_decay[-1:], cum_state[-1:]], axis=1)
    table = lax.all_to_all(
        jnp.broadcast_to(ends, (32, *ends.shape)), SEQ, split_axis=0, concat_axis=0, tiled=True
    )[:, 0]
    width = cum_decay.shape[1]
    _, prefix_state = lax.associative_scan(
        chain_step, (table[:, :width], table[:, width:]), axis=0
    )
    position = z * 4 + y
    previous = lax.dynamic_index_in_dim(
        prefix_state, jnp.maximum(position - 1, 0), 0, keepdims=True
    )
    carried = jnp.where(position > 0, previous, jnp.zeros_like(previous))
    state = cum_decay * carried + cum_state
    mixed = (state * branch_y).astype(BF16)
    own_share = sum_to_owner(spread(ints(dest_at), mixed, out_weight))
    residual = (layer_input.astype(F32) + own_share).astype(BF16)

    order, starts, at = [], [], 0
    for offsets in GROUPS:
        begins = []
        for turn in (0, 1, -1, 2):
            begins.append(at)
            for k in offsets:
                order.append(((z - k) % 8) * 4 + (y - turn) % 4)
                at += 128
        starts.append(begins)
    starts[3].append(starts[3][3] + 256)
    mlp_normed = norm(blocks_of_all(residual), ints(block_at + order), mlp_gain, True)
    total = None
    for number, pieces in enumerate(groups):
        total = up(mlp_normed, pieces, starts[number], total, number == 3)
    slot = []
    for k in OUT_ORDER:
        dest = (z - k) % 8
        slot.append(jnp.where(dest % 2 == c, 0, 4) + (dest // 2 - x) % 4)
    lanes = [(y - turn) % 4 for turn in (0, 1, 2, 3)]
    terms = down(ints(slot + lanes), total, [out_z[k] for k in OUT_ORDER])
    return (residual.astype(F32) + sum_to_owner(terms)).astype(BF16)


def solution(mesh):
    finer = Mesh(mesh.devices.reshape(8, 4, 4, 2), ("z", "y", "x", "c"))
    both = ("x", "c")
    return jax.shard_map(
        shards,
        mesh=finer,
        in_specs=(
            P(SEQ, both),
            P(),
            P(None, None, both),
            P(None, both),
            P(both),
            P(None, both, None, None),
            P(None, both),
            P(both),
            P(both, None),
            P(),
            P(None, SEQ, both),
            P(both, SEQ),
        ),
        out_specs=P(SEQ, both),
        check_vma=False,
    )
```
